32 devices in a mesh: grp: 8 (over z, x), tp: 4 (over y, core).
Axes of the slice: x: 2, y: 2, z: 4, core: 2. Of those that a mesh axis runs over, the one named last changes fastest.
Arguments:
- prefix_keys: bfloat16 [16, 128, 1024], P(None, ('grp', 'tp')), may hold values from -4.5 to 4.5
- prefix_values: bfloat16 [16, 128, 1024], P(None, ('grp', 'tp')), may hold values from -24 to 24
- cand_queries: bfloat16 [8, 4, 256, 8192], P('grp', None, None, 'tp'), may hold values from -120 to 120
- cand_keys: bfloat16 [8, 4, 256, 1024], P('grp', None, None, 'tp'), may hold values from -4.2 to 4.2
- cand_values: bfloat16 [8, 4, 256, 1024], P('grp', None, None, 'tp'), may hold values from -24 to 24
- live_counts: int32 [8], replicated, may hold values from 1 to 4, as said below
- assignment: int32 [8], replicated, may hold values from 0 to 15
Outputs:
- attended: bfloat16 [8, 4, 256, 8192], P('grp', None, None, 'tp')
The draws below stay inside these ranges and needn't reach their ends.
Inputs may be any that keep to these rules, and one draw needn't show every extreme that they name: The live passages of group g fill slots 0 to live_counts[g] - 1; some group has 4, and the group whose index differs from it in the lowest bit has 1.
All inputs are finite; a program needn't handle non-finite values.
Results may differ from the reference program's by a relative error of at most 0.0045.
Values may be sent and summed in bfloat16 or wider, within the bound.
No kernel may reach another device: no remote copies, remote signals or barrier semaphores. Data moves between devices by JAX's collectives and lax.ppermute only.
A program may use at most 64 MiB of HBM per device.

```python
import math
import jax
import jax.numpy as jnp
from jax import lax

HEADS = 64
KV_HEADS = 8
HEAD_DIM = 128
QUERIES = 16
PASS = 256
C_MAX = 4
PREFIX = 128
GROUPS = 8


def drawn_pair(key):
    base = jax.random.fold_in(key, 17)
    key_draw = jax.random.normal(jax.random.fold_in(base, 1), (GROUPS, C_MAX, PASS, KV_HEADS * HEAD_DIM), jnp.float32)
    key_draw = jnp.clip(key_draw, -4.0, 4.0)
    query_draw = 2.0 * jax.random.normal(jax.random.fold_in(base, 2), (GROUPS, C_MAX, PASS, HEADS * HEAD_DIM), jnp.float32)
    query_draw = jnp.clip(query_draw, -8.0, 8.0)
    return (query_draw, key_draw)


def draw_cand_queries(key, part):
    return drawn_pair(key)[0].astype(jnp.bfloat16)


def draw_cand_keys(key, part):
    return drawn_pair(key)[1].astype(jnp.bfloat16)


def draw_live_counts(key, part):
    index = jnp.arange(GROUPS, dtype=jnp.int32)
    selector = jax.random.randint(jax.random.fold_in(key, 5), (GROUPS,), 0, 4, dtype=jnp.int32)
    spread = jax.random.randint(jax.random.fold_in(key, 6), (GROUPS,), 1, C_MAX + 1, dtype=jnp.int32)
    counts = jnp.where(selector == 0, spread, jnp.ones((GROUPS,), jnp.int32))
    busiest = jax.random.randint(jax.random.fold_in(key, 7), (), 0, GROUPS, dtype=jnp.int32)
    counts = jnp.where(index == busiest, jnp.full((GROUPS,), C_MAX, jnp.int32), counts)
    neighbour = jnp.bitwise_xor(busiest, 1)
    counts = jnp.where(index == neighbour, jnp.ones((GROUPS,), jnp.int32), counts)
    return counts.astype(jnp.int32)


def plant(drawn, key, smallest, largest):
    longest = drawn.shape.index(max(drawn.shape))
    spots = []
    for shift in (0, 1):
        where = [jax.random.randint(jax.random.fold_in(key, axis), (), 0, length) for axis, length in enumerate(drawn.shape)]
        where[longest] = (where[longest] + shift) % drawn.shape[longest]
        spots.append(tuple(where))
    return drawn.at[spots[0]].set(smallest).at[spots[1]].set(largest)


def steps_of(rng, shape, pieces, smallest, top_value):
    gain = 1.0
    for position, blocks in pieces:
        draws = jax.random.uniform(jax.random.fold_in(jax.random.fold_in(rng, 6), position), (blocks,), jnp.float32, smallest / len(pieces), top_value / len(pieces))
        gain = gain * jnp.repeat(jnp.exp(draws), shape[position] // blocks).reshape((-1,) + (1,) * (len(shape) - 1 - position))
    return gain


def bell_draw(stream_key, shape, deviation, most, pieces=(), kind=jnp.bfloat16):
    level = steps_of(stream_key, shape, pieces, -0.22, 0.18) if pieces else 1.0
    entries = jax.random.normal(stream_key, shape, jnp.float32) * deviation * level
    return jnp.minimum(jnp.maximum(entries, -most), most).astype(kind)


def setup_inputs(seed: int = 0) -> dict:
    splits = jax.random.split(jax.random.key(seed), 8)
    return {
        "prefix_keys": bell_draw(splits[0], (QUERIES, PREFIX, KV_HEADS * HEAD_DIM), 1.0, 4.5, ((1, 32),)),
        "prefix_values": bell_draw(splits[1], (QUERIES, PREFIX, KV_HEADS * HEAD_DIM), 4.0, 24.0, ((1, 32),)),
        "cand_queries": draw_cand_queries(jax.random.fold_in(splits[7], 71), 0),
        "cand_keys": draw_cand_keys(jax.random.fold_in(splits[7], 71), 0),
        "cand_values": bell_draw(splits[4], (GROUPS, C_MAX, PASS, KV_HEADS * HEAD_DIM), 4.0, 24.0, ((0, 8), (3, 4))),
        "live_counts": draw_live_counts(jax.random.fold_in(splits[7], 71), 0),
        "assignment": plant(jax.random.randint(splits[6], (GROUPS,), 0, QUERIES), jax.random.fold_in(splits[6], 1), 0, QUERIES - 1).astype(jnp.int32),
    }


masked_score = -1e+30

def head_attention(query_rows, keys, values, visible, ratio):
    rows = query_rows.astype(jnp.float32).reshape(query_rows.shape[0], ratio, HEAD_DIM)
    scores = jnp.einsum('prd,kd->rpk', rows, keys.astype(jnp.float32), precision=lax.Precision.HIGHEST)
    scores = scores * (1.0 / math.sqrt(HEAD_DIM))
    scores = jnp.where(visible[None], scores, masked_score)
    peak = lax.optimization_barrier(jnp.max(scores, axis=-1))
    weights = jnp.exp(scores - peak[..., None])
    total = lax.optimization_barrier(jnp.sum(weights, axis=-1))
    rounded = lax.optimization_barrier(weights.astype(jnp.bfloat16)).astype(jnp.float32)
    mixed = jnp.einsum('rpk,kd->prd', rounded, values.astype(jnp.float32), precision=lax.Precision.HIGHEST)
    mixed = mixed / jnp.transpose(total)[:, :, None]
    return mixed.reshape(query_rows.shape[0], ratio * HEAD_DIM)

def reference(prefix_keys, prefix_values, cand_queries, cand_keys, cand_values, live_counts, assignment):
    ratio = HEADS // KV_HEADS
    width = ratio * HEAD_DIM
    key_index = jnp.arange(PREFIX + PASS, dtype=jnp.int32)
    row_index = jnp.arange(PASS, dtype=jnp.int32)
    visible = (key_index[None, :] < PREFIX) | (key_index[None, :] - PREFIX <= row_index[:, None])
    anchor = jnp.zeros((), jnp.int32)

    def one_group(group):
        chosen = assignment[group].astype(jnp.int32)
        front_keys = lax.dynamic_index_in_dim(prefix_keys, chosen, 0, keepdims=False)
        front_values = lax.dynamic_index_in_dim(prefix_values, chosen, 0, keepdims=False)
        queries = lax.dynamic_index_in_dim(cand_queries, group, 0, keepdims=False)
        own_keys = lax.dynamic_index_in_dim(cand_keys, group, 0, keepdims=False)
        own_values = lax.dynamic_index_in_dim(cand_values, group, 0, keepdims=False)

        def one_item(item):
            slot = (item // KV_HEADS).astype(jnp.int32)
            head = (item % KV_HEADS).astype(jnp.int32)
            query_rows = lax.dynamic_slice(queries, (slot, anchor, head * width), (1, PASS, width))[0]
            near_keys = lax.dynamic_slice(own_keys, (slot, anchor, head * HEAD_DIM), (1, PASS, HEAD_DIM))[0]
            near_values = lax.dynamic_slice(own_values, (slot, anchor, head * HEAD_DIM), (1, PASS, HEAD_DIM))[0]
            far_keys = lax.dynamic_slice_in_dim(front_keys, head * HEAD_DIM, HEAD_DIM, 1)
            far_values = lax.dynamic_slice_in_dim(front_values, head * HEAD_DIM, HEAD_DIM, 1)
            keys = jnp.concatenate([far_keys, near_keys], 0)
            values = jnp.concatenate([far_values, near_values], 0)
            return head_attention(query_rows, keys, values, visible, ratio)
        results = lax.map(one_item, jnp.arange(C_MAX * KV_HEADS, dtype=jnp.int32))
        results = results.reshape(C_MAX, KV_HEADS, PASS, width)
        results = jnp.transpose(results, (0, 2, 1, 3)).reshape(C_MAX, PASS, HEADS * HEAD_DIM)
        results = results.astype(jnp.bfloat16)
        alive = jnp.arange(C_MAX, dtype=jnp.int32) < live_counts[group].astype(jnp.int32)
        return jnp.where(alive[:, None, None], results, jnp.zeros_like(results))
    return lax.map(one_group, jnp.arange(GROUPS, dtype=jnp.int32))
```

```python
import math

import jax
import jax.numpy as jnp
from jax import lax
from jax.experimental import pallas as pl
from jax.experimental.pallas import tpu as pltpu
from jax.sharding import PartitionSpec as P

HEAD_DIM = 128
MASKED = -1e30
SCALE = math.log2(math.e) / math.sqrt(HEAD_DIM)
VMEM_LIMIT = 60 * 1024 * 1024
BF16 = jnp.bfloat16
F32 = jnp.float32
NEAR = jnp.float32


def dot_nt(a, b):
    return lax.dot_general(a, b, (((1,), (1,)), ((), ())), preferred_element_type=F32)


def dot_nn(a, b):
    return lax.dot_general(a, b, (((1,), (0,)), ((), ())), preferred_element_type=F32)


def pick_kernel(assign, keys, values, out, sem):
    tp = out.shape[0] // assign.shape[0]
    width = out.shape[3]

    def group(g, carry):
        row = assign[g]
        for t in range(tp):
            for i, src in enumerate((keys, values)):
                pltpu.make_async_copy(
                    src.at[row, :, pl.ds(t * width, width)], out.at[g * tp + t, i], sem
                ).start()
        return carry

    lax.fori_loop(0, assign.shape[0], group, 0)
    pltpu.make_async_copy(out, out, sem).wait()


def query_tile(q, i, pairs):
    d = HEAD_DIM
    return jnp.concatenate(
        [
            jnp.concatenate(
                [q[0, 0, :, p * d : (p + 1) * d], q[0, 0, :, (pairs + p) * d : (pairs + p + 1) * d]],
                axis=1,
            )
            for p in (2 * i, 2 * i + 1)
        ],
        axis=0,
    )


def near_kernel(counts, q, k, v, o, stat, kbd, vtd):
    count = counts[lax.axis_index("grp")]
    s, t = pl.program_id(0), pl.program_id(1)
    half = q.shape[2]
    pairs = q.shape[3] // (2 * HEAD_DIM)
    d = HEAD_DIM

    @pl.when((s == 0) & (t == 0))
    def _():
        kbd[...] = jnp.zeros_like(kbd)
        vtd[...] = jnp.zeros_like(vtd)

    @pl.when((s < count) & (t == 0))
    def _():
        vt = v[0, 0].T
        for b in range(2):
            rows = slice(b * half, (b + 1) * half)
            for h in range(2):
                at = slice((2 * b + h) * half, (2 * b + h + 1) * half)
                cols = slice(h * d, (h + 1) * d)
                kbd[at, cols] = k[0, 0, rows, cols]
                vtd[cols, at] = vt[cols, rows]

    def attend(blocks):
        row = lax.broadcasted_iota(jnp.int32, (half, 2 * half), 0)
        col = lax.broadcasted_iota(jnp.int32, (half, 2 * half), 1)
        seen = row <= jnp.where(col < half, col, col - half)
        keys = kbd[: blocks * 2 * half]
        mixers = vtd[:, : blocks * 2 * half]
        for i in range(pairs // 2):
            scores = dot_nt(keys, query_tile(q, i, pairs))
            weights = [None] * (2 * blocks)
            for h in range(2):
                parts = []
                for b in range(blocks):
                    x = scores[(2 * b + h) * half : (2 * b + h + 1) * half]
                    parts.append(jnp.where(seen, x, MASKED) if b == blocks - 1 else x)
                top = jnp.max(parts[0], axis=0, keepdims=True)
                for x in parts[1:]:
                    top = jnp.maximum(top, jnp.max(x, axis=0, keepdims=True))
                total = None
                for b, x in enumerate(parts):
                    e = jnp.exp2((x - top) * SCALE)
                    part = jnp.sum(e, axis=0, keepdims=True)
                    total = part if total is None else total + part
                    weights[2 * b + h] = e.astype(BF16)
                stat[0, 0, i, h : h + 1, :] = top
                stat[0, 0, i, 2 + h : 3 + h, :] = total
            o[0, 0, i] = dot_nn(mixers, jnp.concatenate(weights, axis=0)).astype(o.dtype)

    @pl.when((s < count) & (t == 0))
    def _():
        attend(1)

    @pl.when((s < count) & (t == 1))
    def _():
        attend(2)


def far_kernel(counts, front, q, o, stat, out, rows, kfd, vfd):
    count = counts[lax.axis_index("grp")]
    s, t = pl.program_id(0), pl.program_id(1)
    half = q.shape[2]
    pairs = q.shape[3] // (2 * HEAD_DIM)
    d = HEAD_DIM
    devices, _, local, _ = front.shape
    prefix = devices * local

    @pl.when((s == 0) & (t == 0))
    def _():
        kfd[...] = jnp.zeros_like(kfd)
        vfd[...] = jnp.zeros_like(vfd)
        for i in range(2):
            for n in range(devices):
                rows[i, n * local : (n + 1) * local, :] = front[n, i].astype(F32)
        for h in range(2):
            cols = slice(h * d, (h + 1) * d)
            at = slice(h * prefix, (h + 1) * prefix)
            kfd[at, cols] = rows[0, :, cols].astype(BF16)
            vfd[cols, at] = rows[1, :, cols].T.astype(BF16)

    @pl.when(s >= count)
    def _():
        out[...] = jnp.zeros_like(out)

    @pl.when(s < count)
    def _():
        for i in range(pairs // 2):
            scores = dot_nt(kfd[...], query_tile(q, i, pairs))
            weights, fades, invs = [], [], []
            for h in range(2):
                x = scores[h * prefix : (h + 1) * prefix]
                m = stat[0, 0, i, h : h + 1, :]
                l = stat[0, 0, i, 2 + h : 3 + h, :]
                top = jnp.maximum(m, jnp.max(x, axis=0, keepdims=True))
                e = jnp.exp2((x - top) * SCALE)
                fade = jnp.exp2((m - top) * SCALE)
                total = l * fade + jnp.sum(e, axis=0, keepdims=True)
                weights.append(e.astype(BF16))
                fades.append(fade)
                invs.append(1.0 / total)
            mixed = dot_nn(vfd[...], jnp.concatenate(weights, axis=0))
            for h in range(2):
                r = slice(h * d, (h + 1) * d)
                y = (mixed[r] + o[0, 0, i, r, :].astype(F32) * fades[h]) * invs[h]
                y = y.astype(BF16).T
                for n in range(2):
                    c = (h * pairs + 2 * i + n) * d
                    out[0, 0, :, c : c + d] = y[n * half : (n + 1) * half]


def per_device(
    prefix_keys, prefix_values, cand_queries, cand_keys, cand_values, live_counts, assignment
):
    _, slots, passage, q_width = cand_queries.shape
    k_width = cand_keys.shape[3]
    local = prefix_keys.shape[1]
    devices = lax.axis_size("grp") * lax.axis_size("tp")
    prefix = devices * local
    pairs = q_width // (2 * HEAD_DIM)
    assert k_width == 2 * HEAD_DIM
    any_space = pl.BlockSpec(memory_space=pl.ANY)
    vmem = pl.BlockSpec(memory_space=pltpu.VMEM)
    smem = pl.BlockSpec(memory_space=pltpu.SMEM)
    picked = pl.pallas_call(
        pick_kernel,
        out_shape=jax.ShapeDtypeStruct((devices, 2, local, k_width), BF16),
        in_specs=[smem, any_space, any_space],
        out_specs=any_space,
        scratch_shapes=[pltpu.SemaphoreType.DMA],
        compiler_params=pltpu.CompilerParams(vmem_limit_bytes=1024 * 1024),
        name="pick",
    )(assignment, prefix_keys, prefix_values)
    front = lax.all_to_all(picked, ("grp", "tp"), split_axis=0, concat_axis=0, tiled=True)

    half = passage // 2
    flops = 4 * slots * passage * q_width * passage
    tile = lambda s, t: (0, s, t, 0)
    whole = lambda s, t: (0, s, 0, 0)
    q_spec = pl.BlockSpec((1, 1, half, q_width), tile)
    kv_spec = pl.BlockSpec((1, 1, passage, k_width), whole)
    o_spec = pl.BlockSpec((1, 1, pairs // 2, k_width, 2 * half), lambda s, t: (s, t, 0, 0, 0))
    stat_spec = pl.BlockSpec((1, 1, pairs // 2, 8, 2 * half), lambda s, t: (s, t, 0, 0, 0))
    o, stat = pl.pallas_call(
        near_kernel,
        out_shape=(
            jax.ShapeDtypeStruct((slots, 2, pairs // 2, k_width, 2 * half), NEAR),
            jax.ShapeDtypeStruct((slots, 2, pairs // 2, 8, 2 * half), F32),
        ),
        grid=(slots, 2),
        in_specs=[smem, q_spec, kv_spec, kv_spec],
        out_specs=(o_spec, stat_spec),
        scratch_shapes=[
            pltpu.VMEM((2 * passage, k_width), BF16),
            pltpu.VMEM((k_width, 2 * passage), BF16),
        ],
        compiler_params=pltpu.CompilerParams(vmem_limit_bytes=VMEM_LIMIT),
        cost_estimate=pl.CostEstimate(flops=flops, transcendentals=0, bytes_accessed=0),
        name="near",
    )(live_counts, cand_queries, cand_keys, cand_values)

    return pl.pallas_call(
        far_kernel,
        out_shape=jax.ShapeDtypeStruct(cand_queries.shape, BF16),
        grid=(slots, 2),
        in_specs=[smem, vmem, q_spec, o_spec, stat_spec],
        out_specs=q_spec,
        scratch_shapes=[
            pltpu.VMEM((2, prefix, k_width), F32),
            pltpu.VMEM((2 * prefix, k_width), BF16),
            pltpu.VMEM((k_width, 2 * prefix), BF16),
        ],
        compiler_params=pltpu.CompilerParams(vmem_limit_bytes=VMEM_LIMIT),
        name="far",
    )(live_counts, front, cand_queries, o, stat)


def solution(mesh):
    placed = (
        P(None, ("grp", "tp"), None),
        P(None, ("grp", "tp"), None),
        P("grp", None, None, "tp"),
        P("grp", None, None, "tp"),
        P("grp", None, None, "tp"),
        P(),
        P(),
    )
    return jax.shard_map(
        per_device,
        mesh=mesh,
        in_specs=placed,
        out_specs=P("grp", None, None, "tp"),
        check_vma=False,
    )
```

```python
import math

import jax
import jax.numpy as jnp
from jax import lax
from jax.experimental import pallas as pl
from jax.experimental.pallas import tpu as pltpu
from jax.sharding import PartitionSpec as P

HEAD_DIM = 128
MASKED = -1e30
LEAD = 16
LEAST, MOST = 2.0**-60, 2.0**120
SCALE = math.log2(math.e) / math.sqrt(HEAD_DIM)
VMEM_LIMIT = 40 * 1024 * 1024
BF16 = jnp.bfloat16
F32 = jnp.float32
NEAR = jnp.bfloat16


def dot_nt(a, b):
    return lax.dot_general(a, b, (((1,), (1,)), ((), ())), preferred_element_type=F32)


def dot_nn(a, b):
    return lax.dot_general(a, b, (((1,), (0,)), ((), ())), preferred_element_type=F32)


def pick_kernel(assign, keys, values, out, ids, kb, vb, sem):
    copies = [
        pltpu.make_async_copy(src, dst, sem.at[i])
        for i, (src, dst) in enumerate(((assign, ids), (keys, kb), (values, vb)))
    ]
    for copy in copies:
        copy.start()
    for copy in copies:
        copy.wait()
    groups = assign.shape[0]
    tp = out.shape[0] // groups
    width = out.shape[3]

    def group(g, carry):
        row = ids[g]
        for i, src in enumerate((kb, vb)):
            for t in range(tp):
                out[g * tp + t, i] = src[row, :, t * width : (t + 1) * width]
        return carry

    lax.fori_loop(0, groups, group, 0, unroll=8)


def query_copies(q, qb, sem, s, i):
    wide = qb.shape[4]
    step = q.shape[3] // 2
    return [
        pltpu.make_async_copy(
            q.at[0, s, :, pl.ds(pl.multiple_of(h * step + i * wide, wide), wide)],
            qb.at[s, i, h],
            sem.at[s, i],
        )
        for h in range(2)
    ]


def arrived(buffer, sem):
    pltpu.make_async_copy(buffer, buffer, sem).wait()


def query_tile(qb, s, i, t):
    half = qb.shape[3] // 2
    d = HEAD_DIM
    rows = slice(t * half, (t + 1) * half)
    return jnp.concatenate(
        [
            jnp.concatenate([qb[s, i, h, rows, n * d : (n + 1) * d] for h in range(2)], axis=1)
            for n in range(2)
        ],
        axis=0,
    )


def staged(count, turns, score, weigh, mix, arrive, leave, ahead):
    load, store = ahead

    def slot(s, carry):
        after = jnp.minimum(s + 1, count - 1)
        arrive(s, after)
        scores, weights = load()
        for i in range(turns):
            if i == 0:
                mix(jnp.maximum(s - 1, 0), turns - 1, weights)
            else:
                mix(s, i - 1, weights)
                leave(s, i - 1)
            following = score(s, i + 1) if i + 1 < turns else score(after, 0)
            weights = weigh(s, i, scores)
            scores = following
        store(scores, weights)
        pl.when(s > 0)(lambda: leave(s - 1, turns - 1))
        return carry

    arrive(None, 0)
    store(score(0, 0), None)
    lax.fori_loop(0, count, slot, 0)
    mix(count - 1, turns - 1, load()[1])
    leave(count - 1, turns - 1)


def near_kernel(
    counts, q, k, v, o, stat, q0, o0,
    ids, qb, kb, vb, ob, kbd, vtd, hidden, nexts, lasts, sc, sq, skv, so, s0,
):
    slots, turns, _, passage, wide = qb.shape
    d = HEAD_DIM
    half = passage // 2
    fetch = pltpu.make_async_copy(counts, ids, sc)
    fetch.start()

    def load(s):
        pltpu.make_async_copy(k.at[0, s], kb.at[s], skv.at[s]).start()
        pltpu.make_async_copy(v.at[0, s], vb.at[s], skv.at[s]).start()

    def load_queries(s):
        for i in range(turns):
            for copy in query_copies(q, qb, sq, s, i):
                copy.start()

    load(0)
    load_queries(0)
    fetch.wait()
    count = ids[lax.axis_index("grp")]
    for s in range(1, slots):
        pl.when(s < count)(lambda s=s: load(s))
    for s in range(1, slots):
        pl.when(s < count)(lambda s=s: load_queries(s))
    firsts = [copy for i in range(turns) for copy in query_copies(q, q0, s0, 0, i)]
    for copy in firsts:
        copy.start()
    row = lax.broadcasted_iota(jnp.int32, (half, 2 * half), 0)
    col = lax.broadcasted_iota(jnp.int32, (half, 2 * half), 1)
    col = jnp.where(col < half, col, col - half)
    hidden[...] = jnp.where(row <= col, 0.0, MASKED)

    def build(s):
        vt = vb[s].T
        gap = jnp.zeros((half, d), BF16)
        tag = lax.broadcasted_iota(jnp.int32, (LEAD, half), 0)
        for b in range(2):
            rows = slice(b * half, (b + 1) * half)
            for h in range(2):
                at = slice((2 * b + h) * half, (2 * b + h + 1) * half)
                for c in range(2):
                    cols = slice(c * d, (c + 1) * d)
                    kbd[s, at, cols] = kb[s, rows, cols] if c == h else gap
                    vtd[s, LEAD + c * d : LEAD + (c + 1) * d, at] = vt[cols, rows] if c == h else gap
                vtd[s, :LEAD, at] = jnp.where(tag == h, 1.0, 0.0).astype(BF16)

    def spans(t):
        first = t * 2 * half
        return slice(first, first + (t + 1) * 2 * half)

    def load_ahead():
        return [nexts[spans(t)] for t in range(2)], [lasts[spans(t)] for t in range(2)]

    def store_ahead(scores, weights):
        for t in range(2):
            nexts[spans(t)] = scores[t]
            if weights is not None:
                lasts[spans(t)] = weights[t]

    def score(s, i):
        return [
            dot_nt(kbd[s, : (t + 1) * 2 * half], query_tile(qb, s, i, t)) for t in range(2)
        ]

    def weigh(s, i, scores):
        result = []
        for t in range(2):
            parts = []
            for r in range(2 * (t + 1)):
                x = scores[t][r * half : (r + 1) * half] * SCALE
                x = x + hidden[...] if r // 2 == t else x
                parts.append(jnp.exp2(x).astype(BF16))
            result.append(jnp.concatenate(parts, axis=0))
        return result

    def mix(s, i, weights):
        for t in range(2):
            mixed = dot_nn(vtd[s, :, : (t + 1) * 2 * half], weights[t])
            stat[s, i, t, 0:2, :] = mixed[0:2]
            ob[s, i, t] = mixed[LEAD:].astype(ob.dtype)

    def leave(s, i):
        pltpu.make_async_copy(ob.at[s, i], o.at[s, i], so.at[s, i]).start()

    def arrive(s, after):
        if s is None:
            arrived(kb.at[0], skv.at[0])
            arrived(vb.at[0], skv.at[0])
            build(0)
            arrived(qb.at[0, 0], sq.at[0, 0])
            return

        for i in range(1, turns):
            arrived(qb.at[s, i], sq.at[s, i])

        @pl.when(s + 1 < count)
        def _():
            arrived(kb.at[after], skv.at[after])
            arrived(vb.at[after], skv.at[after])
            arrived(qb.at[after, 0], sq.at[after, 0])

        build(after)

    staged(count, turns, score, weigh, mix, arrive, leave, (load_ahead, store_ahead))

    def drain(n, carry):
        s, i = n // turns, n % turns
        arrived(ob.at[s, i], so.at[s, i])
        return carry

    o0[...] = ob[0]
    for i in range(turns):
        arrived(q0.at[0, i], s0.at[0, i])
    lax.fori_loop(0, count * turns, drain, 0)


def far_kernel(
    counts, front, q, o, stat, q0, o0, k, v, out,
    ids, qb, ob, yb, rows, kfd, vfd, nexts, lasts, mark, kb, vb, sc, sq, so, sy, skv,
):
    slots, turns, _, passage, wide = qb.shape
    d = HEAD_DIM
    half = passage // 2
    devices, _, local, _ = front.shape
    prefix = devices * local
    fetch = pltpu.make_async_copy(counts, ids, sc)
    fetch.start()

    def load(s):
        for i in range(turns):
            for copy in query_copies(q, qb, sq, s, i):
                copy.start()
            pltpu.make_async_copy(o.at[s, i], ob.at[s, i], so.at[s]).start()

    for s in range(1, slots):
        load(s)
    qb[0] = q0[0]
    ob[0] = o0[...]
    for i in range(2):
        for n in range(devices):
            rows[i, n * local : (n + 1) * local, :] = front[n, i].astype(F32)
    gap = jnp.zeros((prefix, d), BF16)
    tag = lax.broadcasted_iota(jnp.int32, (LEAD, prefix), 0)
    for h in range(2):
        at = slice(h * prefix, (h + 1) * prefix)
        for c in range(2):
            cols = slice(c * d, (c + 1) * d)
            kfd[at, cols] = rows[0, :, cols].astype(BF16) if c == h else gap
            vfd[LEAD + c * d : LEAD + (c + 1) * d, at] = (
                rows[1, :, cols].T.astype(BF16) if c == h else gap.T
            )
        vfd[:LEAD, at] = jnp.where(tag == h, 1.0, 0.0).astype(BF16)

    fetch.wait()
    count = ids[lax.axis_index("grp")]

    def empty(s, carry):
        yb[s] = jnp.zeros(yb.shape[1:], yb.dtype)
        for i in range(turns):
            leave(s, i)
        return carry

    def put(s, i):
        step = out.shape[3] // 2
        return [
            pltpu.make_async_copy(
                yb.at[s, i, h],
                out.at[0, s, :, pl.ds(pl.multiple_of(h * step + i * wide, wide), wide)],
                sy.at[s],
            )
            for h in range(2)
        ]

    def leave(s, i):
        for copy in put(s, i):
            copy.start()

    lax.fori_loop(count, slots, empty, 0)

    def span(t):
        return slice(t * 2 * prefix, (t + 1) * 2 * prefix)

    def load_ahead():
        return [nexts[span(t)] for t in range(2)], [lasts[span(t)] for t in range(2)]

    def store_ahead(scores, weights):
        for t in range(2):
            nexts[span(t)] = scores[t]
            if weights is not None:
                lasts[span(t)] = weights[t]

    def score(s, i):
        return [dot_nt(kfd[...], query_tile(qb, s, i, t)) for t in range(2)]

    def weigh(s, i, scores):
        return [jnp.exp2(x * SCALE).astype(BF16) for x in scores]

    def mix(s, i, weights):
        worst = None
        for t in range(2):
            mixed = dot_nn(vfd[...], weights[t])
            for h in range(2):
                r = slice(h * d, (h + 1) * d)
                total = stat[s, i, t, h : h + 1, :] + mixed[h : h + 1]
                wrong = jnp.where((total > LEAST) & (total < MOST), 0.0, 1.0)
                worst = wrong if worst is None else jnp.maximum(worst, wrong)
                y = mixed[LEAD + h * d : LEAD + (h + 1) * d] + ob[s, i, t, r, :].astype(F32)
                y = y * (1.0 / total)
                y = y.astype(BF16).T
                for n in range(2):
                    yb[s, i, h, t * half : (t + 1) * half, n * d : (n + 1) * d] = y[
                        n * half : (n + 1) * half
                    ]
        mark[s, i : i + 1, :] = worst

    def arrive(s, after):
        if s is None:
            return

        @pl.when(s > 0)
        def _():
            for i in range(1, turns):
                arrived(qb.at[s, i], sq.at[s, i])
            arrived(ob.at[s], so.at[s])

        @pl.when(s + 1 < count)
        def _():
            arrived(qb.at[after, 0], sq.at[after, 0])

    mark[...] = jnp.zeros_like(mark)
    staged(count, turns, score, weigh, mix, arrive, leave, (load_ahead, store_ahead))
    wrong = jnp.max(mark[...]) > 0.0

    def unread(s, carry):
        for i in range(turns):
            arrived(qb.at[s, i], sq.at[s, i])
        arrived(ob.at[s], so.at[s])
        return carry

    lax.fori_loop(count, slots, unread, 0)
    for s in range(slots):
        arrived(yb.at[s], sy.at[s])

    def redo(s, carry):
        own = [
            pltpu.make_async_copy(src.at[0, s], dst, skv.at[j])
            for j, (src, dst) in enumerate(((k, kb), (v, vb)))
        ]
        for copy in own:
            copy.start()
        for copy in own:
            copy.wait()
        row = lax.broadcasted_iota(jnp.int32, (passage, passage), 0)
        col = lax.broadcasted_iota(jnp.int32, (passage, passage), 1)

        def tile(i, carry):
            for h in range(2):
                cols, far = slice(h * d, (h + 1) * d), slice(h * prefix, (h + 1) * prefix)
                for n in range(2):
                    x = qb[s, i, h, :, n * d : (n + 1) * d]
                    near = jnp.where(row <= col, dot_nt(kb[:, cols], x), MASKED)
                    away = dot_nt(kfd[far, cols], x)
                    top = jnp.maximum(
                        jnp.max(near, axis=0, keepdims=True), jnp.max(away, axis=0, keepdims=True)
                    )
                    near = jnp.exp2((near - top) * SCALE)
                    away = jnp.exp2((away - top) * SCALE)
                    total = jnp.sum(near, axis=0, keepdims=True)
                    total = total + jnp.sum(away, axis=0, keepdims=True)
                    y = dot_nn(vb[:, cols].T, near.astype(BF16))
                    y = (y + dot_nn(vfd[LEAD + h * d : LEAD + (h + 1) * d, far], away.astype(BF16))) * (1.0 / total)
                    yb[s, i, h, :, n * d : (n + 1) * d] = y.astype(BF16).T
            return carry

        lax.fori_loop(0, turns, tile, 0)
        for i in range(turns):
            leave(s, i)
        arrived(yb.at[s], sy.at[s])
        return carry

    @pl.when(wrong)
    def _():
        lax.fori_loop(0, count, redo, 0)


def per_device(
    prefix_keys, prefix_values, cand_queries, cand_keys, cand_values, live_counts, assignment
):
    _, slots, passage, q_width = cand_queries.shape
    k_width = cand_keys.shape[3]
    local = prefix_keys.shape[1]
    devices = lax.axis_size("grp") * lax.axis_size("tp")
    prefix = devices * local
    pairs = q_width // (2 * HEAD_DIM)
    assert k_width == 2 * HEAD_DIM
    half = passage // 2
    turns = pairs // 2
    assert pairs % 2 == 0
    in_hbm = lambda x: pltpu.with_memory_space_constraint(x, pltpu.HBM)
    hbm = pl.BlockSpec(memory_space=pltpu.HBM)
    vmem = pl.BlockSpec(memory_space=pltpu.VMEM)
    dma = pltpu.SemaphoreType.DMA
    params = pltpu.CompilerParams(vmem_limit_bytes=VMEM_LIMIT)
    counts, queries = in_hbm(live_counts), in_hbm(cand_queries)
    own = in_hbm(cand_keys), in_hbm(cand_values)
    picked = pl.pallas_call(
        pick_kernel,
        out_shape=jax.ShapeDtypeStruct((devices, 2, local, k_width), BF16),
        in_specs=[hbm, hbm, hbm],
        out_specs=vmem,
        scratch_shapes=[
            pltpu.SMEM(assignment.shape, jnp.int32),
            pltpu.VMEM(prefix_keys.shape, BF16),
            pltpu.VMEM(prefix_values.shape, BF16),
            dma((3,)),
        ],
        compiler_params=params,
        name="pick",
    )(in_hbm(assignment), in_hbm(prefix_keys), in_hbm(prefix_values))
    front = lax.all_to_all(picked, ("grp", "tp"), split_axis=0, concat_axis=0, tiled=True)

    flops = 4 * slots * passage * q_width * passage
    o_shape = (slots, turns, 2, k_width, 2 * half)
    stat_shape = (slots, turns, 2, 8, 2 * half)
    ids = pltpu.SMEM(live_counts.shape, jnp.int32)
    q_buffer = pltpu.VMEM((slots, turns, 2, passage, 2 * HEAD_DIM), BF16)
    kv_buffer = pltpu.VMEM((slots, passage, k_width), BF16)
    o, stat, q0, o0 = pl.pallas_call(
        near_kernel,
        out_shape=(
            pltpu.HBM(o_shape, NEAR),
            jax.ShapeDtypeStruct(stat_shape, F32),
            jax.ShapeDtypeStruct((1, turns, 2, passage, 2 * HEAD_DIM), BF16),
            jax.ShapeDtypeStruct(o_shape[1:], NEAR),
        ),
        in_specs=[hbm, hbm, hbm, hbm],
        out_specs=(hbm, vmem, vmem, vmem),
        scratch_shapes=[
            ids,
            q_buffer,
            kv_buffer,
            kv_buffer,
            pltpu.VMEM(o_shape, NEAR),
            pltpu.VMEM((slots, 2 * passage, k_width), BF16),
            pltpu.VMEM((slots, k_width + LEAD, 2 * passage), BF16),
            pltpu.VMEM((half, 2 * half), F32),
            pltpu.VMEM((6 * half, 2 * half), F32),
            pltpu.VMEM((6 * half, 2 * half), BF16),
            dma,
            dma((slots, turns)),
            dma((slots,)),
            dma((slots, turns)),
            dma((1, turns)),
        ],
        compiler_params=params,
        cost_estimate=pl.CostEstimate(flops=flops, transcendentals=0, bytes_accessed=0),
        name="near",
    )(counts, queries, *own)

    return pl.pallas_call(
        far_kernel,
        out_shape=jax.ShapeDtypeStruct(cand_queries.shape, BF16),
        in_specs=[hbm, vmem, hbm, hbm, vmem, vmem, vmem, hbm, hbm],
        out_specs=hbm,
        scratch_shapes=[
            ids,
            q_buffer,
            pltpu.VMEM(o_shape, NEAR),
            q_buffer,
            pltpu.VMEM((2, prefix, k_width), F32),
            pltpu.VMEM((2 * prefix, k_width), BF16),
            pltpu.VMEM((k_width + LEAD, 2 * prefix), BF16),
            pltpu.VMEM((4 * prefix, 2 * half), F32),
            pltpu.VMEM((4 * prefix, 2 * half), BF16),
            pltpu.VMEM((slots, 8, 2 * half), F32),
            pltpu.VMEM((passage, k_width), BF16),
            pltpu.VMEM((passage, k_width), BF16),
            dma,
            dma((slots, turns)),
            dma((slots,)),
            dma((slots,)),
            dma((2,)),
        ],
        compiler_params=params,
        name="far",
    )(counts, front, queries, in_hbm(o), stat, q0, o0, *own)


def solution(mesh):
    placed = (
        P(None, ("grp", "tp"), None),
        P(None, ("grp", "tp"), None),
        P("grp", None, None, "tp"),
        P("grp", None, None, "tp"),
        P("grp", None, None, "tp"),
        P(),
        P(),
    )
    return jax.shard_map(
        per_device,
        mesh=mesh,
        in_specs=placed,
        out_specs=P("grp", None, None, "tp"),
        check_vma=False,
    )
```

```python
import math

import jax
import jax.numpy as jnp
from jax import lax
from jax.experimental import pallas as pl
from jax.experimental.pallas import tpu as pltpu
from jax.sharding import PartitionSpec as P

HEAD_DIM = 128
MASKED = -1e30
LEAD = 16
LEAST, MOST = 2.0**-60, 2.0**120
SCALE = math.log2(math.e) / math.sqrt(HEAD_DIM)
VMEM_LIMIT = 40 * 1024 * 1024
BF16 = jnp.bfloat16
F32 = jnp.float32
NEAR = jnp.bfloat16


def dot_nt(a, b):
    return lax.dot_general(a, b, (((1,), (1,)), ((), ())), preferred_element_type=F32)


def dot_nn(a, b):
    return lax.dot_general(a, b, (((1,), (0,)), ((), ())), preferred_element_type=F32)


def pick_kernel(assign, keys, values, out, ids, kb, vb, sem):
    copies = [
        pltpu.make_async_copy(src, dst, sem.at[i])
        for i, (src, dst) in enumerate(((assign, ids), (keys, kb), (values, vb)))
    ]
    for copy in copies:
        copy.start()
    for copy in copies:
        copy.wait()
    groups = assign.shape[0]
    tp = out.shape[0] // groups
    width = out.shape[3]

    def group(g, carry):
        row = ids[g]
        for i, src in enumerate((kb, vb)):
            for t in range(tp):
                out[g * tp + t, i] = src[row, :, t * width : (t + 1) * width]
        return carry

    lax.fori_loop(0, groups, group, 0, unroll=8)


def query_copies(q, qb, sem, s, i, row=None):
    wide = qb.shape[-1]
    step = q.shape[3] // 2
    return [
        pltpu.make_async_copy(
            q.at[0, s, :, pl.ds(pl.multiple_of(h * step + i * wide, wide), wide)],
            qb.at[s, i, h] if row is None else qb.at[row, h],
            sem.at[s, i] if row is None else sem.at[row],
        )
        for h in range(2)
    ]


def arrived(buffer, sem):
    pltpu.make_async_copy(buffer, buffer, sem).wait()


def query_tile(qb, s, i, t):
    half = qb.shape[3] // 2
    d = HEAD_DIM
    rows = slice(t * half, (t + 1) * half)
    return jnp.concatenate(
        [
            jnp.concatenate([qb[s, i, h, rows, n * d : (n + 1) * d] for h in range(2)], axis=1)
            for n in range(2)
        ],
        axis=0,
    )


def staged(more, turns, score, weigh, mix, arrive, leave, ahead, leave_soon):
    load, store = ahead

    def slot(s, carry):
        after = jnp.minimum(s + 1, count - 1)
        arrive(s, after)
        scores, weights = load()
        for i in range(turns):
            if i == 0:
                mix(jnp.maximum(s - 1, 0), turns - 1, weights)
            else:
                mix(s, i - 1, weights)
                if leave_soon:
                    leave(s, i - 1)
            following = score(s, i + 1) if i + 1 < turns else score(after, 0)
            weights = weigh(s, i, scores)
            scores = following
        store(scores, weights)

        @pl.when(s > 0)
        def _():
            if leave_soon:
                leave(s - 1, turns - 1)
            else:
                pl.when(s > 1)(lambda: leave(s - 1, turns - 1))
                for i in range(turns - 1):
                    leave(s, i)

        return carry

    arrive(None, 0)
    store(score(0, 0), None)
    count = more()
    lax.fori_loop(0, count, slot, 0)
    mix(count - 1, turns - 1, load()[1])
    if leave_soon:
        leave(count - 1, turns - 1)
    else:
        pl.when(count > 1)(lambda: leave(count - 1, turns - 1))
    return count


def near_kernel(
    counts, q, k, v, o, stat, q0, o0,
    ids, qb, kb, vb, ob, kbd, vtd, hidden, nexts, lasts, sc, sq, skv, so, s0,
):
    slots, turns, _, passage, wide = qb.shape
    d = HEAD_DIM
    half = passage // 2
    fetch = pltpu.make_async_copy(counts, ids, sc)
    fetch.start()

    def load(s):
        pltpu.make_async_copy(k.at[0, s], kb.at[s], skv.at[s]).start()
        pltpu.make_async_copy(v.at[0, s], vb.at[s], skv.at[s]).start()

    def load_queries(s):
        for i in range(turns):
            for copy in query_copies(q, qb, sq, s, i):
                copy.start()

    load(0)
    load_queries(0)
    for s in range(1, slots):
        load(s)
    for s in range(1, slots):
        load_queries(s)
    row = lax.broadcasted_iota(jnp.int32, (half, 2 * half), 0)
    col = lax.broadcasted_iota(jnp.int32, (half, 2 * half), 1)
    col = jnp.where(col < half, col, col - half)
    hidden[...] = jnp.where(row <= col, 0.0, MASKED)

    def more():
        fetch.wait()
        count = ids[lax.axis_index("grp")]
        for copy in query_copies(q, q0, s0, 1, 0, turns):
            copy.start()
        for i in range(turns):
            for copy in query_copies(q, q0, s0, 0, i, i):
                copy.start()
        return count

    def build(s):
        vt = vb[s].T
        gap = jnp.zeros((half, d), BF16)
        tag = lax.broadcasted_iota(jnp.int32, (LEAD, half), 0)
        for b in range(2):
            rows = slice(b * half, (b + 1) * half)
            for h in range(2):
                at = slice((2 * b + h) * half, (2 * b + h + 1) * half)
                for c in range(2):
                    cols = slice(c * d, (c + 1) * d)
                    kbd[s, at, cols] = kb[s, rows, cols] if c == h else gap
                    vtd[s, LEAD + c * d : LEAD + (c + 1) * d, at] = vt[cols, rows] if c == h else gap
                vtd[s, :LEAD, at] = jnp.where(tag == h, 1.0, 0.0).astype(BF16)

    def spans(t):
        first = t * 2 * half
        return slice(first, first + (t + 1) * 2 * half)

    def load_ahead():
        return [nexts[spans(t)] for t in range(2)], [lasts[spans(t)] for t in range(2)]

    def store_ahead(scores, weights):
        for t in range(2):
            nexts[spans(t)] = scores[t]
            if weights is not None:
                lasts[spans(t)] = weights[t]

    def score(s, i):
        return [
            dot_nt(kbd[s, : (t + 1) * 2 * half], query_tile(qb, s, i, t)) for t in range(2)
        ]

    def weigh(s, i, scores):
        result = []
        for t in range(2):
            parts = []
            for r in range(2 * (t + 1)):
                x = scores[t][r * half : (r + 1) * half] * SCALE
                x = x + hidden[...] if r // 2 == t else x
                parts.append(jnp.exp2(x).astype(BF16))
            result.append(jnp.concatenate(parts, axis=0))
        return result

    def mix(s, i, weights):
        for t in range(2):
            mixed = dot_nn(vtd[s, :, : (t + 1) * 2 * half], weights[t])
            stat[s, i, t, 0:2, :] = mixed[0:2]
            ob[s, i, t] = mixed[LEAD:].astype(ob.dtype)

    def leave(s, i):
        pltpu.make_async_copy(ob.at[s, i], o.at[s, i], so.at[s, i]).start()

    def arrive(s, after):
        if s is None:
            arrived(kb.at[0], skv.at[0])
            arrived(vb.at[0], skv.at[0])
            build(0)
            arrived(qb.at[0, 0], sq.at[0, 0])
            return

        count = ids[lax.axis_index("grp")]
        for i in range(1, turns):
            arrived(qb.at[s, i], sq.at[s, i])

        @pl.when(s + 1 < count)
        def _():
            arrived(kb.at[after], skv.at[after])
            arrived(vb.at[after], skv.at[after])
            arrived(qb.at[after, 0], sq.at[after, 0])

        build(after)

    ahead = (load_ahead, store_ahead)
    count = staged(more, turns, score, weigh, mix, arrive, leave, ahead, False)

    def unread(s, carry):
        arrived(kb.at[s], skv.at[s])
        arrived(vb.at[s], skv.at[s])
        for i in range(turns):
            arrived(qb.at[s, i], sq.at[s, i])
        return carry

    lax.fori_loop(count, slots, unread, 0)

    def drain(n, carry):
        s, i = n // turns, n % turns
        arrived(ob.at[s, i], so.at[s, i])
        return carry

    o0[...] = ob[0]
    for i in range(turns + 1):
        arrived(q0.at[i], s0.at[i])
    lax.fori_loop(turns, count * turns, drain, 0)


def far_kernel(
    counts, front, q, o, stat, q0, o0, k, v, out,
    ids, qb, ob, yb, rows, kfd, vfd, nexts, lasts, mark, kb, vb, sc, sq, so, sy, skv,
):
    slots, turns, _, passage, wide = qb.shape
    d = HEAD_DIM
    half = passage // 2
    devices, _, local, _ = front.shape
    prefix = devices * local
    fetch = pltpu.make_async_copy(counts, ids, sc)
    fetch.start()

    def load(s):
        for i in range(turns):
            if (s, i) != (1, 0):
                for copy in query_copies(q, qb, sq, s, i):
                    copy.start()
            pltpu.make_async_copy(o.at[s, i], ob.at[s, i], so.at[s]).start()

    load(1)

    for i in range(2):
        for n in range(devices):
            rows[i, n * local : (n + 1) * local, :] = front[n, i].astype(F32)
    gap = jnp.zeros((prefix, d), BF16)
    tag = lax.broadcasted_iota(jnp.int32, (LEAD, prefix), 0)
    for h in range(2):
        at = slice(h * prefix, (h + 1) * prefix)
        for c in range(2):
            cols = slice(c * d, (c + 1) * d)
            kfd[at, cols] = rows[0, :, cols].astype(BF16) if c == h else gap
            vfd[LEAD + c * d : LEAD + (c + 1) * d, at] = (
                rows[1, :, cols].T.astype(BF16) if c == h else gap.T
            )
        vfd[:LEAD, at] = jnp.where(tag == h, 1.0, 0.0).astype(BF16)

    def more():
        fetch.wait()
        count = ids[lax.axis_index("grp")]
        for s in range(2, slots):
            pl.when(s < count)(lambda s=s: load(s))
        lax.fori_loop(count, slots, empty, 0)
        return count

    def empty(s, carry):
        yb[s] = jnp.zeros(yb.shape[1:], yb.dtype)
        for i in range(turns):
            leave(s, i)
        return carry

    def put(s, i):
        step = out.shape[3] // 2
        return [
            pltpu.make_async_copy(
                yb.at[s, i, h],
                out.at[0, s, :, pl.ds(pl.multiple_of(h * step + i * wide, wide), wide)],
                sy.at[s],
            )
            for h in range(2)
        ]

    def leave(s, i):
        for copy in put(s, i):
            copy.start()

    def span(t):
        return slice(t * 2 * prefix, (t + 1) * 2 * prefix)

    def load_ahead():
        return [nexts[span(t)] for t in range(2)], [lasts[span(t)] for t in range(2)]

    def store_ahead(scores, weights):
        for t in range(2):
            nexts[span(t)] = scores[t]
            if weights is not None:
                lasts[span(t)] = weights[t]

    def score(s, i):
        return [dot_nt(kfd[...], query_tile(qb, s, i, t)) for t in range(2)]

    def weigh(s, i, scores):
        return [jnp.exp2(x * SCALE).astype(BF16) for x in scores]

    def mix(s, i, weights):
        worst = None
        for t in range(2):
            mixed = dot_nn(vfd[...], weights[t])
            for h in range(2):
                r = slice(h * d, (h + 1) * d)
                total = stat[s, i, t, h : h + 1, :] + mixed[h : h + 1]
                wrong = jnp.where((total > LEAST) & (total < MOST), 0.0, 1.0)
                worst = wrong if worst is None else jnp.maximum(worst, wrong)
                y = mixed[LEAD + h * d : LEAD + (h + 1) * d] + ob[s, i, t, r, :].astype(F32)
                y = y * (1.0 / total)
                y = y.astype(BF16).T
                for n in range(2):
                    yb[s, i, h, t * half : (t + 1) * half, n * d : (n + 1) * d] = y[
                        n * half : (n + 1) * half
                    ]
        mark[s, i : i + 1, :] = worst

    def arrive(s, after):
        if s is None:
            return

        count = ids[lax.axis_index("grp")]

        @pl.when(s > 0)
        def _():
            for i in range(1, turns):
                arrived(qb.at[s, i], sq.at[s, i])
            arrived(ob.at[s], so.at[s])

        @pl.when((s > 0) & (s + 1 < count))
        def _():
            arrived(qb.at[after, 0], sq.at[after, 0])

    def keep():
        qb[0] = q0[:turns]
        qb[1, 0] = q0[turns]
        ob[0] = o0[...]
        mark[...] = jnp.zeros_like(mark)
        return more()

    count = keep()
    ahead = (load_ahead, store_ahead)
    staged(lambda: count, turns, score, weigh, mix, arrive, leave, ahead, True)
    wrong = jnp.max(mark[...]) > 0.0

    @pl.when(count == 1)
    def _():
        for i in range(1, turns):
            arrived(qb.at[1, i], sq.at[1, i])
        arrived(ob.at[1], so.at[1])
    for s in range(slots):
        arrived(yb.at[s], sy.at[s])

    def redo(s, carry):
        own = [
            pltpu.make_async_copy(src.at[0, s], dst, skv.at[j])
            for j, (src, dst) in enumerate(((k, kb), (v, vb)))
        ]
        for copy in own:
            copy.start()
        for copy in own:
            copy.wait()
        row = lax.broadcasted_iota(jnp.int32, (passage, passage), 0)
        col = lax.broadcasted_iota(jnp.int32, (passage, passage), 1)

        def tile(i, carry):
            for h in range(2):
                cols, far = slice(h * d, (h + 1) * d), slice(h * prefix, (h + 1) * prefix)
                for n in range(2):
                    x = qb[s, i, h, :, n * d : (n + 1) * d]
                    near = jnp.where(row <= col, dot_nt(kb[:, cols], x), MASKED)
                    away = dot_nt(kfd[far, cols], x)
                    top = jnp.maximum(
                        jnp.max(near, axis=0, keepdims=True), jnp.max(away, axis=0, keepdims=True)
                    )
                    near = jnp.exp2((near - top) * SCALE)
                    away = jnp.exp2((away - top) * SCALE)
                    total = jnp.sum(near, axis=0, keepdims=True)
                    total = total + jnp.sum(away, axis=0, keepdims=True)
                    y = dot_nn(vb[:, cols].T, near.astype(BF16))
                    y = (y + dot_nn(vfd[LEAD + h * d : LEAD + (h + 1) * d, far], away.astype(BF16))) * (1.0 / total)
                    yb[s, i, h, :, n * d : (n + 1) * d] = y.astype(BF16).T
            return carry

        lax.fori_loop(0, turns, tile, 0)
        for i in range(turns):
            leave(s, i)
        arrived(yb.at[s], sy.at[s])
        return carry

    @pl.when(wrong)
    def _():
        lax.fori_loop(0, count, redo, 0)


def per_device(
    prefix_keys, prefix_values, cand_queries, cand_keys, cand_values, live_counts, assignment
):
    _, slots, passage, q_width = cand_queries.shape
    k_width = cand_keys.shape[3]
    local = prefix_keys.shape[1]
    devices = lax.axis_size("grp") * lax.axis_size("tp")
    prefix = devices * local
    pairs = q_width // (2 * HEAD_DIM)
    assert k_width == 2 * HEAD_DIM
    half = passage // 2
    turns = pairs // 2
    assert pairs % 2 == 0 and slots > 1
    in_hbm = lambda x: pltpu.with_memory_space_constraint(x, pltpu.HBM)
    hbm = pl.BlockSpec(memory_space=pltpu.HBM)
    vmem = pl.BlockSpec(memory_space=pltpu.VMEM)
    dma = pltpu.SemaphoreType.DMA
    params = pltpu.CompilerParams(vmem_limit_bytes=VMEM_LIMIT)
    counts, queries = in_hbm(live_counts), in_hbm(cand_queries)
    own = in_hbm(cand_keys), in_hbm(cand_values)
    picked = pl.pallas_call(
        pick_kernel,
        out_shape=jax.ShapeDtypeStruct((devices, 2, local, k_width), BF16),
        in_specs=[hbm, hbm, hbm],
        out_specs=vmem,
        scratch_shapes=[
            pltpu.SMEM(assignment.shape, jnp.int32),
            pltpu.VMEM(prefix_keys.shape, BF16),
            pltpu.VMEM(prefix_values.shape, BF16),
            dma((3,)),
        ],
        compiler_params=params,
        name="pick",
    )(in_hbm(assignment), in_hbm(prefix_keys), in_hbm(prefix_values))
    front = lax.all_to_all(picked, ("grp", "tp"), split_axis=0, concat_axis=0, tiled=True)

    flops = 4 * slots * passage * q_width * passage
    o_shape = (slots, turns, 2, k_width, 2 * half)
    stat_shape = (slots, turns, 2, 8, 2 * half)
    ids = pltpu.SMEM(live_counts.shape, jnp.int32)
    q_buffer = pltpu.VMEM((slots, turns, 2, passage, 2 * HEAD_DIM), BF16)
    kv_buffer = pltpu.VMEM((slots, passage, k_width), BF16)
    o, stat, q0, o0 = pl.pallas_call(
        near_kernel,
        out_shape=(
            pltpu.HBM(o_shape, NEAR),
            jax.ShapeDtypeStruct(stat_shape, F32),
            jax.ShapeDtypeStruct((turns + 1, 2, passage, 2 * HEAD_DIM), BF16),
            jax.ShapeDtypeStruct(o_shape[1:], NEAR),
        ),
        in_specs=[hbm, hbm, hbm, hbm],
        out_specs=(hbm, vmem, vmem, vmem),
        scratch_shapes=[
            ids,
            q_buffer,
            kv_buffer,
            kv_buffer,
            pltpu.VMEM(o_shape, NEAR),
            pltpu.VMEM((slots, 2 * passage, k_width), BF16),
            pltpu.VMEM((slots, k_width + LEAD, 2 * passage), BF16),
            pltpu.VMEM((half, 2 * half), F32),
            pltpu.VMEM((6 * half, 2 * half), F32),
            pltpu.VMEM((6 * half, 2 * half), BF16),
            dma,
            dma((slots, turns)),
            dma((slots,)),
            dma((slots, turns)),
            dma((turns + 1,)),
        ],
        compiler_params=params,
        cost_estimate=pl.CostEstimate(flops=flops, transcendentals=0, bytes_accessed=0),
        name="near",
    )(counts, queries, *own)

    return pl.pallas_call(
        far_kernel,
        out_shape=jax.ShapeDtypeStruct(cand_queries.shape, BF16),
        in_specs=[hbm, vmem, hbm, hbm, vmem, vmem, vmem, hbm, hbm],
        out_specs=hbm,
        scratch_shapes=[
            ids,
            q_buffer,
            pltpu.VMEM(o_shape, NEAR),
            q_buffer,
            pltpu.VMEM((2, prefix, k_width), F32),
            pltpu.VMEM((2 * prefix, k_width), BF16),
            pltpu.VMEM((k_width + LEAD, 2 * prefix), BF16),
            pltpu.VMEM((4 * prefix, 2 * half), F32),
            pltpu.VMEM((4 * prefix, 2 * half), BF16),
            pltpu.VMEM((slots, 8, 2 * half), F32),
            pltpu.VMEM((passage, k_width), BF16),
            pltpu.VMEM((passage, k_width), BF16),
            dma,
            dma((slots, turns)),
            dma((slots,)),
            dma((slots,)),
            dma((2,)),
        ],
        compiler_params=params,
        name="far",
    )(counts, front, queries, in_hbm(o), stat, q0, o0, *own)


def solution(mesh):
    placed = (
        P(None, ("grp", "tp"), None),
        P(None, ("grp", "tp"), None),
        P("grp", None, None, "tp"),
        P("grp", None, None, "tp"),
        P("grp", None, None, "tp"),
        P(),
        P(),
    )
    return jax.shard_map(
        per_device,
        mesh=mesh,
        in_specs=placed,
        out_specs=P("grp", None, None, "tp"),
        check_vma=False,
    )
```
